768 devices in a mesh: replica: 8 (over y_lo, core), shard: 96 (over z, y_hi, x).
Axes of the slice: x: 4, y: 8 (y_hi: 2, y_lo: 4; y = y_hi * 4 + y_lo), z: 12, core: 2. Of those that a mesh axis runs over, the one named last changes fastest.
Arguments:
- anchor: float32 [4608, 8192], P('shard'), may hold values from -6 to 6
- replica_rows: bfloat16 [8, 4608, 8192], P('replica', 'shard'), may hold values from -6 to 6
- outer_velocity: float32 [4608, 8192], P('shard', 'replica'), may hold values from -6 to 6
- features: bfloat16 [8, 4608, 3072], P('replica', 'shard'), may hold values from -6 to 6
- cotangent: bfloat16 [8, 3072, 1024], P('replica', 'shard'), may hold values from -0.109375 to 0.109375
- inner_weight: float32 [8, 4608, 1024], P('replica', 'shard'), may hold values from -6 to 6
- first_moment: float32 [8, 4608, 1024], P('replica', 'shard'), may hold values from -6 to 6
- second_moment: float32 [8, 4608, 1024], P('replica', 'shard'), may hold values from 0.5 to 2
Outputs:
- new_anchor: float32 [4608, 8192], P('shard')
- merged_rows: bfloat16 [8, 4608, 8192], P('replica', 'shard')
- new_velocity: float32 [4608, 8192], P('shard', 'replica')
- new_weight: float32 [8, 4608, 1024], P('replica', 'shard')
- new_first: float32 [8, 4608, 1024], P('replica', 'shard')
- new_second: float32 [8, 4608, 1024], P('replica', 'shard')
The draws below stay inside these ranges and needn't reach their ends.
All inputs are finite; a program needn't handle non-finite values.
Results may differ from the reference program's by a relative error of at most 0.0035.
Values may be sent and summed in bfloat16 or wider, within the bound.
No kernel may reach another device: no remote copies, remote signals or barrier semaphores. Data moves between devices by JAX's collectives and lax.ppermute only.
A program may use at most 64 MiB of HBM per device.

```python
import math
import jax
import jax.numpy as jnp
from jax import lax

D = 8192
KV = 1024
DW = 4608
TOK = 3072
N_REPLICA = 8


def shard_levels(stream_key, dims, split, smallest, high):
    def one(axis_at, parts):
        heights = jax.random.uniform(jax.random.fold_in(jax.random.fold_in(stream_key, 6), axis_at), (parts,), jnp.float32, smallest / len(split), high / len(split))
        return jnp.repeat(jnp.exp(heights), dims[axis_at] // parts).reshape((-1,) + (1,) * (len(dims) - axis_at - 1))

    level = one(*split[0])
    for cut in split[1:]:
        level = level * one(*cut)
    return level


def centred(key, extent, width, reach, shards=(), kind=jnp.bfloat16):
    factor_of = shard_levels(key, extent, shards, -0.22, 0.18) if shards else 1.0
    array = jax.random.normal(key, extent, jnp.float32) * width * factor_of
    return jnp.minimum(jnp.maximum(array, -reach), reach).astype(kind)


def setup_inputs(seed: int = 0) -> dict:
    splits = jax.random.split(jax.random.key(seed), 9)
    return {
        "anchor": centred(splits[0], (DW, D), 1.0, 6.0, ((0, 96),), jnp.float32),
        "replica_rows": centred(splits[1], (N_REPLICA, DW, D), 1.0, 6.0, ((0, 8), (1, 96))),
        "outer_velocity": centred(splits[2], (DW, D), 0.5, 6.0, ((0, 96), (1, 8)), jnp.float32),
        "features": centred(splits[3], (N_REPLICA, DW, TOK), 1.0, 6.0, ((0, 8), (1, 96))),
        "cotangent": centred(splits[4], (N_REPLICA, TOK, KV), TOK ** -0.5, 0.109375, ((0, 8), (1, 96))),
        "inner_weight": centred(splits[5], (N_REPLICA, DW, KV), 1.0, 6.0, ((0, 8), (1, 96)), jnp.float32),
        "first_moment": centred(splits[6], (N_REPLICA, DW, KV), 0.5, 6.0, ((0, 8), (1, 96)), jnp.float32),
        "second_moment": jnp.clip(jnp.exp(math.log(2.0) - 1.3862944 * jax.random.uniform(splits[7], (N_REPLICA, DW, KV), jnp.float32) ** shard_levels(splits[7], (N_REPLICA, DW, KV), ((0, 8), (1, 96)), -0.2, 0.2)), 0.5, 2.0),
    }


momentum_keep = 0.9
outer_rate = 0.7
blend_keep = 0.5
inner_rate = 0.01
decay_first = 0.9
decay_second = 0.95
weight_decay = 0.1
epsilon = 1e-08
first_fix = 1.0 - 0.9 ** 10
second_fix = 1.0 - 0.95 ** 10

def reference(anchor, replica_rows, outer_velocity, features, cotangent, inner_weight, first_moment, second_moment):
    drift = anchor[None] - replica_rows.astype(jnp.float32)
    outer_grad = lax.optimization_barrier(jnp.sum(drift, axis=0)) / N_REPLICA
    new_velocity = momentum_keep * outer_velocity + outer_grad
    new_anchor = anchor - outer_rate * (outer_grad + momentum_keep * new_velocity)
    merged_rows = (blend_keep * replica_rows.astype(jnp.float32) + (1.0 - blend_keep) * new_anchor[None]).astype(jnp.bfloat16)
    gradient = jnp.einsum('rdt,rtk->rdk', features.astype(jnp.float32), cotangent.astype(jnp.float32), precision=lax.Precision.HIGHEST)
    new_first = decay_first * first_moment + (1.0 - decay_first) * gradient
    new_second = decay_second * second_moment + (1.0 - decay_second) * gradient * gradient
    stepped = new_first / first_fix / (jnp.sqrt(new_second / second_fix) + epsilon)
    new_weight = inner_weight - inner_rate * (stepped + weight_decay * inner_weight)
    return (new_anchor, merged_rows, new_velocity, new_weight, new_first, new_second)
```

```python
import jax
import jax.numpy as jnp
from jax import lax
from jax.experimental import pallas as pl
from jax.experimental.pallas import tpu as pltpu
from jax.sharding import Mesh
from jax.sharding import PartitionSpec as P

REPLICA = ("y_near", "core")
SHARD = ("z_pair", "z_bit", "y_far", "x")
GROUP = ("z_bit", "x")


momentum_keep = 0.9
outer_rate = 0.7
blend_keep = 0.5
inner_rate = 0.01
decay_first = 0.9
decay_second = 0.95
weight_decay = 0.1
epsilon = 1e-08
first_fix = 1.0 - 0.9**10
second_fix = 1.0 - 0.95**10

LANES = 128


def pack_kernel(features_ref, out_ref):
    rows, tokens = features_ref.shape
    piece = LANES // 4
    lane = lax.broadcasted_iota(jnp.int32, (rows, LANES), 1)
    for block in range(tokens // (8 * LANES)):
        for bit in range(2):
            tiles = []
            for place in range(4):
                column = (block * 2 + place // 2) * 4 + bit * 2 + place % 2
                tiles.append(features_ref[:, column * LANES : (column + 1) * LANES].astype(jnp.float32))
            for x in range(4):
                packed = jnp.zeros((rows, LANES), jnp.float32)
                for place in range(4):
                    shift = (place - x) * piece % LANES
                    turned = pltpu.roll(tiles[place], shift, 1) if shift else tiles[place]
                    packed = jnp.where(lane // piece == place, turned, packed)
                out_ref[bit * 4 + x, :, block * LANES : (block + 1) * LANES] = packed.astype(jnp.bfloat16)


def packed_by_token(features):
    rows, tokens = features.shape
    return pl.pallas_call(
        pack_kernel,
        out_shape=jax.ShapeDtypeStruct((8, rows, tokens // 8), jnp.bfloat16),
        name="pack",
    )(features)


def exchange(x, axes):
    return lax.all_to_all(x, axes, 0, 0, tiled=True)


def local(
    anchor,
    replica_rows,
    outer_velocity,
    features,
    cotangent,
    inner_weight,
    first_moment,
    second_moment,
):
    replicas = lax.axis_size(REPLICA)
    rows = replica_rows[0]
    height, width = rows.shape
    part = outer_velocity.shape[1]

    packed = packed_by_token(features[0])
    other = lax.ppermute(cotangent[0], "y_far", [(0, 1), (1, 0)])
    own_tokens = exchange(packed, GROUP)
    own_tokens = own_tokens.reshape(-1, own_tokens.shape[-1])

    first = lax.axis_index("y_far") == 0
    both = jnp.where(
        first,
        jnp.concatenate([cotangent[0], other]),
        jnp.concatenate([other, cotangent[0]]),
    )
    pieces = jnp.moveaxis(rows.reshape(height, replicas, part), 1, 0)
    pieces, own_tokens, both = lax.optimization_barrier((pieces, own_tokens, both))
    pieces = exchange(pieces, REPLICA)

    own_cotangent = lax.all_gather(both, "z_pair", axis=0, tiled=True)

    partial = jnp.dot(own_tokens, own_cotangent, preferred_element_type=jnp.float32)
    partial = partial.astype(jnp.bfloat16).reshape(-1, height, partial.shape[1])
    partial, pieces = lax.optimization_barrier((partial, pieces))
    parts = exchange(partial, GROUP)

    offset = lax.axis_index(REPLICA) * part
    anchor_part = lax.dynamic_slice_in_dim(anchor, offset, part, 1)
    outer_grad = jnp.sum(anchor_part[None] - pieces.astype(jnp.float32), axis=0) / replicas
    new_velocity = momentum_keep * outer_velocity + outer_grad
    moved = anchor_part - outer_rate * (outer_grad + momentum_keep * new_velocity)
    moved = lax.all_gather(moved.astype(jnp.bfloat16), REPLICA, axis=0)
    new_anchor = jnp.moveaxis(moved, 0, 1).reshape(height, width).astype(jnp.float32)
    merged_rows = (blend_keep * rows.astype(jnp.float32) + (1.0 - blend_keep) * new_anchor).astype(jnp.bfloat16)

    gradient = jnp.sum(parts.astype(jnp.float32), axis=0)[None]
    new_first = decay_first * first_moment + (1.0 - decay_first) * gradient
    new_second = decay_second * second_moment + (1.0 - decay_second) * gradient * gradient
    stepped = new_first / first_fix / (jnp.sqrt(new_second / second_fix) + epsilon)
    new_weight = inner_weight - inner_rate * (stepped + weight_decay * inner_weight)
    return (new_anchor, merged_rows[None], new_velocity, new_weight, new_first, new_second)


def solution(mesh):
    split = Mesh(
        mesh.devices.reshape(4, 2, 6, 2, 2, 4),
        REPLICA + SHARD,
    )
    return jax.shard_map(
        local,
        mesh=split,
        in_specs=(
            P(SHARD, None),
            P(REPLICA, SHARD, None),
            P(SHARD, REPLICA),
            P(REPLICA, SHARD, None),
            P(REPLICA, SHARD, None),
            P(REPLICA, SHARD, None),
            P(REPLICA, SHARD, None),
            P(REPLICA, SHARD, None),
        ),
        out_specs=(
            P(SHARD, None),
            P(REPLICA, SHARD, None),
            P(SHARD, REPLICA),
            P(REPLICA, SHARD, None),
            P(REPLICA, SHARD, None),
            P(REPLICA, SHARD, None),
        ),
        check_vma=False,
    )
```

```python
import jax
import jax.numpy as jnp
from jax import lax
from jax.experimental import pallas as pl
from jax.experimental.pallas import tpu as pltpu
from jax.sharding import Mesh
from jax.sharding import PartitionSpec as P

REPLICA = ("y_near", "core")
SHARD = ("z_pair", "z_bit", "y_far", "x")
GROUP = ("z_bit", "x")


momentum_keep = 0.9
outer_rate = 0.7
blend_keep = 0.5
inner_rate = 0.01
decay_first = 0.9
decay_second = 0.95
weight_decay = 0.1
epsilon = 1e-08
first_fix = 1.0 - 0.9**10
second_fix = 1.0 - 0.95**10

LANES = 128


def pack_kernel(features_ref, out_ref):
    rows, tokens = features_ref.shape
    piece = LANES // 4
    lane = lax.broadcasted_iota(jnp.int32, (rows, LANES), 1)
    for block in range(tokens // (8 * LANES)):
        for bit in range(2):
            tiles = []
            for place in range(4):
                column = (block * 2 + place // 2) * 4 + bit * 2 + place % 2
                tiles.append(features_ref[:, column * LANES : (column + 1) * LANES].astype(jnp.float32))
            for x in range(4):
                packed = jnp.zeros((rows, LANES), jnp.float32)
                for place in range(4):
                    shift = (place - x) * piece % LANES
                    turned = pltpu.roll(tiles[place], shift, 1) if shift else tiles[place]
                    packed = jnp.where(lane // piece == place, turned, packed)
                out_ref[bit * 4 + x, :, block * LANES : (block + 1) * LANES] = packed.astype(jnp.bfloat16)


def packed_by_token(features):
    rows, tokens = features.shape
    return pl.pallas_call(
        pack_kernel,
        out_shape=jax.ShapeDtypeStruct((8, rows, tokens // 8), jnp.bfloat16),
        name="pack",
    )(features)


def split_kernel(rows_ref, out_ref, sems):
    count, _, part = out_ref.shape
    copies = [
        pltpu.make_async_copy(rows_ref.at[:, pl.ds(j * part, part)], out_ref.at[j], sems.at[j])
        for j in range(count)
    ]
    for copy in copies:
        copy.start()
    for copy in copies:
        copy.wait()


def split_by_column(rows, part):
    height, width = rows.shape
    return pl.pallas_call(
        split_kernel,
        in_specs=[pl.BlockSpec(memory_space=pltpu.VMEM)],
        out_specs=pl.BlockSpec(memory_space=pl.ANY),
        out_shape=jax.ShapeDtypeStruct((width // part, height, part), rows.dtype),
        scratch_shapes=[pltpu.SemaphoreType.DMA((width // part,))],
        name="split",
    )(rows)


def finish_kernel(
    moved_ref,
    rows_ref,
    parts_ref,
    weight_ref,
    first_ref,
    second_ref,
    anchor_out,
    merged_out,
    weight_out,
    first_out,
    second_out,
    anchor_buf,
    merged_buf,
    state_buf,
    sems,
):
    count, height, part = moved_ref.shape
    copies = []

    def send(source, target):
        copy = pltpu.make_async_copy(source, target, sems.at[len(copies)])
        copy.start()
        copies.append(copy)

    for j in range(count):
        columns = pl.ds(j * part, part)
        new_anchor = moved_ref[j].astype(jnp.float32)
        anchor_buf[:, columns] = new_anchor
        send(anchor_buf.at[:, columns], anchor_out.at[:, columns])
        merged = blend_keep * rows_ref[:, columns].astype(jnp.float32) + (1.0 - blend_keep) * new_anchor
        merged_buf[:, columns] = merged.astype(jnp.bfloat16)
        send(merged_buf.at[:, columns], merged_out.at[:, columns])
    for top in range(0, height, 16):
        lines = pl.ds(top, 16)
        gradient = parts_ref[0, lines].astype(jnp.float32)
        for k in range(1, parts_ref.shape[0]):
            gradient = gradient + parts_ref[k, lines].astype(jnp.float32)
        new_first = decay_first * first_ref[lines] + (1.0 - decay_first) * gradient
        new_second = decay_second * second_ref[lines] + (1.0 - decay_second) * gradient * gradient
        stepped = new_first / first_fix / (jnp.sqrt(new_second / second_fix) + epsilon)
        weight = weight_ref[lines]
        state_buf[0, lines] = weight - inner_rate * (stepped + weight_decay * weight)
        state_buf[1, lines] = new_first
        state_buf[2, lines] = new_second
    send(state_buf.at[0], weight_out)
    send(state_buf.at[1], first_out)
    send(state_buf.at[2], second_out)
    for copy in copies:
        copy.wait()


def finish(moved, rows, parts, weight, first, second):
    height, width = rows.shape
    whole = jax.ShapeDtypeStruct((height, width), jnp.float32)
    state = jax.ShapeDtypeStruct(weight.shape, jnp.float32)
    kept = pl.BlockSpec(memory_space=pltpu.VMEM)
    far = pl.BlockSpec(memory_space=pl.ANY)
    return pl.pallas_call(
        finish_kernel,
        in_specs=[kept] * 6,
        out_specs=[far] * 5,
        out_shape=[whole, jax.ShapeDtypeStruct(rows.shape, rows.dtype), state, state, state],
        scratch_shapes=[
            pltpu.VMEM((height, width), jnp.float32),
            pltpu.VMEM((height, width), jnp.bfloat16),
            pltpu.VMEM((3, *weight.shape), jnp.float32),
            pltpu.SemaphoreType.DMA((2 * moved.shape[0] + 3,)),
        ],
        name="finish",
    )(moved, rows, parts, weight, first, second)


def exchange(x, axes):
    return lax.all_to_all(x, axes, 0, 0, tiled=True)


def local(
    anchor,
    replica_rows,
    outer_velocity,
    features,
    cotangent,
    inner_weight,
    first_moment,
    second_moment,
):
    replicas = lax.axis_size(REPLICA)
    rows = replica_rows[0]
    height, _ = rows.shape
    part = outer_velocity.shape[1]
    mine = cotangent[0]

    other = lax.ppermute(mine, "y_far", [(0, 1), (1, 0)])
    packed = packed_by_token(features[0])
    own_tokens = exchange(packed, GROUP)

    pieces = split_by_column(rows, part)
    offset = lax.axis_index(REPLICA) * part
    anchor_part = lax.dynamic_slice_in_dim(anchor, offset, part, 1)
    both = jnp.where(lax.axis_index("y_far") == 0, jnp.concatenate([mine, other]), jnp.concatenate([other, mine]))
    pieces, own_tokens, both, anchor_part = lax.optimization_barrier((pieces, own_tokens, both, anchor_part))

    pieces = exchange(pieces, REPLICA)

    own_cotangent = lax.all_gather(both, "z_pair", axis=0, tiled=True)
    own_tokens = own_tokens.reshape(-1, own_tokens.shape[-1])
    partial = jnp.dot(own_tokens, own_cotangent, preferred_element_type=jnp.float32)
    partial = partial.astype(jnp.bfloat16).reshape(-1, height, partial.shape[1])
    partial, pieces = lax.optimization_barrier((partial, pieces))
    parts = exchange(partial, GROUP)

    outer_grad = jnp.sum(anchor_part[None] - pieces.astype(jnp.float32), axis=0) / replicas
    new_velocity = momentum_keep * outer_velocity + outer_grad
    moved = anchor_part - outer_rate * (outer_grad + momentum_keep * new_velocity)
    moved = lax.all_gather(moved.astype(jnp.bfloat16), REPLICA, axis=0)

    new_anchor, merged_rows, new_weight, new_first, new_second = finish(
        moved, rows, parts, inner_weight[0], first_moment[0], second_moment[0]
    )
    return (new_anchor, merged_rows[None], new_velocity, new_weight[None], new_first[None], new_second[None])


def solution(mesh):
    split = Mesh(
        mesh.devices.reshape(4, 2, 6, 2, 2, 4),
        REPLICA + SHARD,
    )
    return jax.shard_map(
        local,
        mesh=split,
        in_specs=(
            P(SHARD, None),
            P(REPLICA, SHARD, None),
            P(SHARD, REPLICA),
            P(REPLICA, SHARD, None),
            P(REPLICA, SHARD, None),
            P(REPLICA, SHARD, None),
            P(REPLICA, SHARD, None),
            P(REPLICA, SHARD, None),
        ),
        out_specs=(
            P(SHARD, None),
            P(REPLICA, SHARD, None),
            P(SHARD, REPLICA),
            P(REPLICA, SHARD, None),
            P(REPLICA, SHARD, None),
            P(REPLICA, SHARD, None),
        ),
        check_vma=False,
    )
```

```python
import jax
import jax.numpy as jnp
from jax import lax
from jax.experimental import pallas as pl
from jax.experimental.pallas import tpu as pltpu
from jax.sharding import Mesh
from jax.sharding import PartitionSpec as P

REPLICA = ("y_near", "core")
SHARD = ("z_pair", "z_bit", "y_far", "x")
GROUP = ("z_bit", "x")


momentum_keep = 0.9
outer_rate = 0.7
blend_keep = 0.5
inner_rate = 0.01
decay_first = 0.9
decay_second = 0.95
weight_decay = 0.1
epsilon = 1e-08
first_fix = 1.0 - 0.9**10
second_fix = 1.0 - 0.95**10

LANES = 128


def start_all(copies):
    for copy in copies:
        copy.start()
    return copies


def prepare_kernel(
    features_ref, rows_ref, packed_out, pieces_out, features_buf, rows_buf, packed_buf, in_sems, out_sems
):
    height, tokens = features_ref.shape
    count, _, part = pieces_out.shape
    features_in = pltpu.make_async_copy(features_ref, features_buf, in_sems.at[count])
    features_in.start()
    columns = [pl.ds(j * part, part) for j in range(count)]
    rows_in = start_all(
        [pltpu.make_async_copy(rows_ref.at[:, columns[j]], rows_buf.at[:, columns[j]], in_sems.at[j]) for j in range(count)]
    )
    piece = LANES // 4
    lane = lax.broadcasted_iota(jnp.int32, (height, LANES), 1)
    features_in.wait()
    for block in range(tokens // (8 * LANES)):
        for bit in range(2):
            tiles = []
            for place in range(4):
                column = (block * 2 + place // 2) * 4 + bit * 2 + place % 2
                tiles.append(features_buf[:, column * LANES : (column + 1) * LANES].astype(jnp.float32))
            for x in range(4):
                packed = jnp.zeros((height, LANES), jnp.float32)
                for place in range(4):
                    shift = (place - x) * piece % LANES
                    turned = pltpu.roll(tiles[place], shift, 1) if shift else tiles[place]
                    packed = jnp.where(lane // piece == place, turned, packed)
                packed_buf[bit * 4 + x, :, block * LANES : (block + 1) * LANES] = packed.astype(jnp.bfloat16)
    copies = start_all([pltpu.make_async_copy(packed_buf, packed_out, out_sems.at[count])])
    for j in range(count):
        rows_in[j].wait()
        copies += start_all([pltpu.make_async_copy(rows_buf.at[:, columns[j]], pieces_out.at[j], out_sems.at[j])])
    for copy in copies:
        copy.wait()


def prepare(features, rows, part):
    height, width = rows.shape
    tokens = features.shape[1]
    count = width // part
    far = pl.BlockSpec(memory_space=pl.ANY)
    return pl.pallas_call(
        prepare_kernel,
        in_specs=[far] * 2,
        out_specs=[far] * 2,
        out_shape=[
            jax.ShapeDtypeStruct((8, height, tokens // 8), jnp.bfloat16),
            jax.ShapeDtypeStruct((count, height, part), rows.dtype),
        ],
        scratch_shapes=[
            pltpu.VMEM(features.shape, features.dtype),
            pltpu.VMEM(rows.shape, rows.dtype),
            pltpu.VMEM((8, height, tokens // 8), jnp.bfloat16),
            pltpu.SemaphoreType.DMA((count + 1,)),
            pltpu.SemaphoreType.DMA((count + 1,)),
        ],
        name="prepare",
    )(features, rows)


def exchange(x, axes):
    return lax.all_to_all(x, axes, 0, 0, tiled=True)


def local(
    anchor,
    replica_rows,
    outer_velocity,
    features,
    cotangent,
    inner_weight,
    first_moment,
    second_moment,
):
    replicas = lax.axis_size(REPLICA)
    rows = replica_rows[0]
    height, _ = rows.shape
    part = outer_velocity.shape[1]
    mine = cotangent[0]

    packed, pieces = prepare(features[0], rows, part)
    own_tokens = exchange(packed, GROUP)
    other = lax.ppermute(mine, "y_far", [(0, 1), (1, 0)])

    offset = lax.axis_index(REPLICA) * part
    anchor_part = lax.dynamic_slice_in_dim(anchor, offset, part, 1)
    pieces, own_tokens, anchor_part = lax.optimization_barrier((pieces, own_tokens, anchor_part))

    pieces = exchange(pieces, REPLICA)

    both = jnp.where(
        lax.axis_index("y_far") == 0,
        jnp.concatenate([mine, other]),
        jnp.concatenate([other, mine]),
    )
    own_cotangent = lax.all_gather(both, "z_pair", axis=0, tiled=True)
    own_tokens = own_tokens.reshape(-1, own_tokens.shape[-1])
    partial = jnp.dot(own_tokens, own_cotangent, preferred_element_type=jnp.float32)
    partial = partial.astype(jnp.bfloat16).reshape(-1, height, partial.shape[1])
    partial, pieces = lax.optimization_barrier((partial, pieces))
    parts = exchange(partial, GROUP)

    outer_grad = jnp.sum(anchor_part[None] - pieces.astype(jnp.float32), axis=0) / replicas
    new_velocity = momentum_keep * outer_velocity + outer_grad
    moved = anchor_part - outer_rate * (outer_grad + momentum_keep * new_velocity)
    moved = lax.all_gather(moved.astype(jnp.bfloat16), REPLICA, axis=1, tiled=True)

    new_anchor = moved.astype(jnp.float32)
    merged_rows = (blend_keep * rows.astype(jnp.float32) + (1.0 - blend_keep) * new_anchor).astype(jnp.bfloat16)

    gradient = jnp.sum(parts.astype(jnp.float32), axis=0)[None]
    new_first = decay_first * first_moment + (1.0 - decay_first) * gradient
    new_second = decay_second * second_moment + (1.0 - decay_second) * gradient * gradient
    stepped = new_first / first_fix / (jnp.sqrt(new_second / second_fix) + epsilon)
    new_weight = inner_weight - inner_rate * (stepped + weight_decay * inner_weight)
    return (new_anchor, merged_rows[None], new_velocity, new_weight, new_first, new_second)


def solution(mesh):
    split = Mesh(
        mesh.devices.reshape(4, 2, 6, 2, 2, 4),
        REPLICA + SHARD,
    )
    return jax.shard_map(
        local,
        mesh=split,
        in_specs=(
            P(SHARD, None),
            P(REPLICA, SHARD, None),
            P(SHARD, REPLICA),
            P(REPLICA, SHARD, None),
            P(REPLICA, SHARD, None),
            P(REPLICA, SHARD, None),
            P(REPLICA, SHARD, None),
            P(REPLICA, SHARD, None),
        ),
        out_specs=(
            P(SHARD, None),
            P(REPLICA, SHARD, None),
            P(SHARD, REPLICA),
            P(REPLICA, SHARD, None),
            P(REPLICA, SHARD, None),
            P(REPLICA, SHARD, None),
        ),
        check_vma=False,
    )
```

```python
import jax
import jax.numpy as jnp
from jax import lax
from jax.experimental import pallas as pl
from jax.experimental.pallas import tpu as pltpu
from jax.sharding import Mesh
from jax.sharding import PartitionSpec as P

REPLICA = ("y_near", "core")
SHARD = ("z_pair", "z_bit", "y_far", "x")
GROUP = ("x", "z_bit")


momentum_keep = 0.9
outer_rate = 0.7
blend_keep = 0.5
inner_rate = 0.01
decay_first = 0.9
decay_second = 0.95
weight_decay = 0.1
epsilon = 1e-08
first_fix = 1.0 - 0.9**10
second_fix = 1.0 - 0.95**10

LANES = 128


def start_all(copies):
    for copy in copies:
        copy.start()
    return copies


def prepare_kernel(
    features_ref, rows_ref, packed_out, pieces_out, features_buf, rows_buf, packed_buf, in_sems, out_sems
):
    height, tokens = features_ref.shape
    count, _, part = pieces_out.shape
    features_in = pltpu.make_async_copy(features_ref, features_buf, in_sems.at[count])
    features_in.start()
    columns = [pl.ds(j * part, part) for j in range(count)]
    rows_in = start_all(
        [pltpu.make_async_copy(rows_ref.at[:, columns[j]], rows_buf.at[:, columns[j]], in_sems.at[j]) for j in range(count)]
    )
    piece = LANES // 4
    lane = lax.broadcasted_iota(jnp.int32, (height, LANES), 1)
    features_in.wait()
    for block in range(tokens // (8 * LANES)):
        for bit in range(2):
            tiles = []
            for place in range(4):
                column = (block * 2 + place // 2) * 4 + bit * 2 + place % 2
                tiles.append(features_buf[:, column * LANES : (column + 1) * LANES].astype(jnp.float32))
            for x in range(4):
                packed = jnp.zeros((height, LANES), jnp.float32)
                for place in range(4):
                    shift = (place - x) * piece % LANES
                    turned = pltpu.roll(tiles[place], shift, 1) if shift else tiles[place]
                    packed = jnp.where(lane // piece == place, turned, packed)
                packed_buf[x * 2 + bit, :, block * LANES : (block + 1) * LANES] = packed.astype(jnp.bfloat16)
    copies = start_all([pltpu.make_async_copy(packed_buf, packed_out, out_sems.at[count])])
    for j in range(count):
        rows_in[j].wait()
        copies += start_all([pltpu.make_async_copy(rows_buf.at[:, columns[j]], pieces_out.at[j % 2 * (count // 2) + j // 2], out_sems.at[j])])
    for copy in copies:
        copy.wait()


def prepare(features, rows, part):
    height, width = rows.shape
    tokens = features.shape[1]
    count = width // part
    far = pl.BlockSpec(memory_space=pl.ANY)
    return pl.pallas_call(
        prepare_kernel,
        in_specs=[far] * 2,
        out_specs=[far] * 2,
        out_shape=[
            jax.ShapeDtypeStruct((8, height, tokens // 8), jnp.bfloat16),
            jax.ShapeDtypeStruct((count, height, part), rows.dtype),
        ],
        scratch_shapes=[
            pltpu.VMEM(features.shape, features.dtype),
            pltpu.VMEM(rows.shape, rows.dtype),
            pltpu.VMEM((8, height, tokens // 8), jnp.bfloat16),
            pltpu.SemaphoreType.DMA((count + 1,)),
            pltpu.SemaphoreType.DMA((count + 1,)),
        ],
        name="prepare",
    )(features, rows)


def exchange(x, axes):
    return lax.all_to_all(x, axes, 0, 0, tiled=True)


def local(
    anchor,
    replica_rows,
    outer_velocity,
    features,
    cotangent,
    inner_weight,
    first_moment,
    second_moment,
):
    replicas = lax.axis_size(REPLICA)
    rows = replica_rows[0]
    height, _ = rows.shape
    part = outer_velocity.shape[1]
    mine = cotangent[0]

    packed, pieces = prepare(features[0], rows, part)
    own_tokens = exchange(packed, GROUP)
    other = lax.ppermute(mine, "y_far", [(0, 1), (1, 0)])

    offset = lax.axis_index(REPLICA) * part
    anchor_part = lax.dynamic_slice_in_dim(anchor, offset, part, 1)
    pieces, own_tokens, anchor_part = lax.optimization_barrier((pieces, own_tokens, anchor_part))

    pieces = exchange(pieces, REPLICA[::-1])

    both = jnp.where(
        lax.axis_index("y_far") == 0,
        jnp.concatenate([mine, other]),
        jnp.concatenate([other, mine]),
    )
    own_cotangent = lax.all_gather(both, "z_pair", axis=0, tiled=True)
    own_tokens = own_tokens.reshape(-1, own_tokens.shape[-1])
    partial = jnp.dot(own_tokens, own_cotangent, preferred_element_type=jnp.float32)
    partial = partial.astype(jnp.bfloat16).reshape(-1, height, partial.shape[1])
    partial, pieces = lax.optimization_barrier((partial, pieces))
    parts = exchange(partial, GROUP)

    outer_grad = jnp.sum(anchor_part[None] - pieces.astype(jnp.float32), axis=0) / replicas
    new_velocity = momentum_keep * outer_velocity + outer_grad
    moved = anchor_part - outer_rate * (outer_grad + momentum_keep * new_velocity)
    moved = lax.all_gather(moved.astype(jnp.bfloat16), REPLICA, axis=1, tiled=True)

    gradient = jnp.sum(parts.astype(jnp.float32), axis=0)[None]
    new_first = decay_first * first_moment + (1.0 - decay_first) * gradient
    new_second = decay_second * second_moment + (1.0 - decay_second) * gradient * gradient
    stepped = new_first / first_fix / (jnp.sqrt(new_second / second_fix) + epsilon)
    new_weight = inner_weight - inner_rate * (stepped + weight_decay * inner_weight)

    moved, new_weight, new_first, new_second = lax.optimization_barrier((moved, new_weight, new_first, new_second))
    new_anchor = moved.astype(jnp.float32)
    merged_rows = (blend_keep * rows.astype(jnp.float32) + (1.0 - blend_keep) * new_anchor).astype(jnp.bfloat16)
    return (new_anchor, merged_rows[None], new_velocity, new_weight, new_first, new_second)


def solution(mesh):
    split = Mesh(
        mesh.devices.reshape(4, 2, 6, 2, 2, 4),
        REPLICA + SHARD,
    )
    return jax.shard_map(
        local,
        mesh=split,
        in_specs=(
            P(SHARD, None),
            P(REPLICA, SHARD, None),
            P(SHARD, REPLICA),
            P(REPLICA, SHARD, None),
            P(REPLICA, SHARD, None),
            P(REPLICA, SHARD, None),
            P(REPLICA, SHARD, None),
            P(REPLICA, SHARD, None),
        ),
        out_specs=(
            P(SHARD, None),
            P(REPLICA, SHARD, None),
            P(SHARD, REPLICA),
            P(REPLICA, SHARD, None),
            P(REPLICA, SHARD, None),
            P(REPLICA, SHARD, None),
        ),
        check_vma=False,
    )
```

```python
import jax
import jax.numpy as jnp
from jax import lax
from jax.experimental import pallas as pl
from jax.experimental.pallas import tpu as pltpu
from jax.sharding import Mesh
from jax.sharding import PartitionSpec as P

REPLICA = ("y_near", "core")
SHARD = ("z_pair", "z_bit", "y_far", "x")
GROUP = ("x", "z_bit")


momentum_keep = 0.9
outer_rate = 0.7
blend_keep = 0.5
inner_rate = 0.01
decay_first = 0.9
decay_second = 0.95
weight_decay = 0.1
epsilon = 1e-08
first_fix = 1.0 - 0.9**10
second_fix = 1.0 - 0.95**10

LANES = 128


def start_all(copies):
    for copy in copies:
        copy.start()
    return copies


def prepare_kernel(
    features_ref, rows_ref, packed_out, pieces_out, features_buf, rows_buf, packed_buf, in_sems, out_sems
):
    height, tokens = features_ref.shape
    count, _, part = pieces_out.shape
    blocks = tokens // (8 * LANES)
    wide = [pl.ds(block * 8 * LANES, 8 * LANES) for block in range(blocks)]
    features_in = start_all(
        [
            pltpu.make_async_copy(features_ref.at[:, wide[k]], features_buf.at[:, wide[k]], in_sems.at[count + k])
            for k in range(blocks)
        ]
    )
    columns = [pl.ds(j * part, part) for j in range(count)]
    rows_in = start_all(
        [pltpu.make_async_copy(rows_ref.at[:, columns[j]], rows_buf.at[:, columns[j]], in_sems.at[j]) for j in range(count)]
    )
    piece = LANES // 4
    lane = lax.broadcasted_iota(jnp.int32, (height, LANES), 1)
    copies = []
    for block in range(blocks):
        features_in[block].wait()
        for bit in range(2):
            tiles = []
            for place in range(4):
                column = (block * 2 + place // 2) * 4 + bit * 2 + place % 2
                tiles.append(features_buf[:, column * LANES : (column + 1) * LANES].astype(jnp.float32))
            for x in range(4):
                packed = jnp.zeros((height, LANES), jnp.float32)
                for place in range(4):
                    shift = (place - x) * piece % LANES
                    turned = pltpu.roll(tiles[place], shift, 1) if shift else tiles[place]
                    packed = jnp.where(lane // piece == place, turned, packed)
                packed_buf[x * 2 + bit, :, block * LANES : (block + 1) * LANES] = packed.astype(jnp.bfloat16)
        lanes = pl.ds(block * LANES, LANES)
        copies += start_all(
            [pltpu.make_async_copy(packed_buf.at[:, :, lanes], packed_out.at[:, :, lanes], out_sems.at[count + block])]
        )
    for j in range(count):
        rows_in[j].wait()
        copies += start_all([pltpu.make_async_copy(rows_buf.at[:, columns[j]], pieces_out.at[j % 2 * (count // 2) + j // 2], out_sems.at[j])])
    for copy in copies:
        copy.wait()


def prepare(features, rows, part):
    height, width = rows.shape
    tokens = features.shape[1]
    count = width // part
    far = pl.BlockSpec(memory_space=pl.ANY)
    return pl.pallas_call(
        prepare_kernel,
        in_specs=[far] * 2,
        out_specs=[far] * 2,
        out_shape=[
            jax.ShapeDtypeStruct((8, height, tokens // 8), jnp.bfloat16),
            jax.ShapeDtypeStruct((count, height, part), rows.dtype),
        ],
        scratch_shapes=[
            pltpu.VMEM(features.shape, features.dtype),
            pltpu.VMEM(rows.shape, rows.dtype),
            pltpu.VMEM((8, height, tokens // 8), jnp.bfloat16),
            pltpu.SemaphoreType.DMA((count + tokens // (8 * LANES),)),
            pltpu.SemaphoreType.DMA((count + tokens // (8 * LANES),)),
        ],
        name="prepare",
    )(features, rows)


def exchange(x, axes):
    return lax.all_to_all(x, axes, 0, 0, tiled=True)


def local(
    anchor,
    replica_rows,
    outer_velocity,
    features,
    cotangent,
    inner_weight,
    first_moment,
    second_moment,
):
    replicas = lax.axis_size(REPLICA)
    rows = replica_rows[0]
    height, _ = rows.shape
    part = outer_velocity.shape[1]
    mine = cotangent[0]

    packed, pieces = prepare(features[0], rows, part)
    own_tokens = exchange(packed, GROUP)
    other = lax.ppermute(mine, "y_far", [(0, 1), (1, 0)])

    offset = lax.axis_index(REPLICA) * part
    anchor_part = lax.dynamic_slice_in_dim(anchor, offset, part, 1)
    pieces, own_tokens, anchor_part = lax.optimization_barrier((pieces, own_tokens, anchor_part))

    pieces = exchange(pieces, REPLICA[::-1])

    both = jnp.where(
        lax.axis_index("y_far") == 0,
        jnp.concatenate([mine, other]),
        jnp.concatenate([other, mine]),
    )
    own_cotangent = lax.all_gather(both, "z_pair", axis=0, tiled=True)
    own_tokens = own_tokens.reshape(-1, own_tokens.shape[-1])
    partial = jnp.dot(own_tokens, own_cotangent, preferred_element_type=jnp.float32)
    partial = partial.astype(jnp.bfloat16).reshape(-1, height, partial.shape[1])
    partial, pieces = lax.optimization_barrier((partial, pieces))
    parts = exchange(partial, GROUP)

    outer_grad = jnp.sum(anchor_part[None] - pieces.astype(jnp.float32), axis=0) / replicas
    new_velocity = momentum_keep * outer_velocity + outer_grad
    moved = anchor_part - outer_rate * (outer_grad + momentum_keep * new_velocity)
    moved = lax.all_gather(moved.astype(jnp.bfloat16), REPLICA, axis=1, tiled=True)

    new_anchor = moved.astype(jnp.float32)
    merged_rows = (blend_keep * rows.astype(jnp.float32) + (1.0 - blend_keep) * new_anchor).astype(jnp.bfloat16)

    gradient = jnp.sum(parts.astype(jnp.float32), axis=0)[None]
    new_first = decay_first * first_moment + (1.0 - decay_first) * gradient
    new_second = decay_second * second_moment + (1.0 - decay_second) * gradient * gradient
    stepped = new_first / first_fix / (jnp.sqrt(new_second / second_fix) + epsilon)
    new_weight = inner_weight - inner_rate * (stepped + weight_decay * inner_weight)
    return (new_anchor, merged_rows[None], new_velocity, new_weight, new_first, new_second)


def solution(mesh):
    split = Mesh(
        mesh.devices.reshape(4, 2, 6, 2, 2, 4),
        REPLICA + SHARD,
    )
    return jax.shard_map(
        local,
        mesh=split,
        in_specs=(
            P(SHARD, None),
            P(REPLICA, SHARD, None),
            P(SHARD, REPLICA),
            P(REPLICA, SHARD, None),
            P(REPLICA, SHARD, None),
            P(REPLICA, SHARD, None),
            P(REPLICA, SHARD, None),
            P(REPLICA, SHARD, None),
        ),
        out_specs=(
            P(SHARD, None),
            P(REPLICA, SHARD, None),
            P(SHARD, REPLICA),
            P(REPLICA, SHARD, None),
            P(REPLICA, SHARD, None),
            P(REPLICA, SHARD, None),
        ),
        check_vma=False,
    )
```
